32 devices in a mesh: replica: 8 (over z, y), model: 4 (over x, core).
Axes of the slice: x: 2, y: 2, z: 4, core: 2. Of those that a mesh axis runs over, the one named last changes fastest.
Arguments:
- slope_query: bfloat16 [8, 1024, 1024], P('replica', None, 'model'), may hold values from -4 to 4
- slope_key: bfloat16 [8, 1024, 1024], P('replica', None, 'model'), may hold values from -4 to 4
- slope_value: bfloat16 [8, 1024, 1024], P('replica', None, 'model'), may hold values from -4 to 4
- slope_mixed: bfloat16 [8, 1024, 1024], P('replica', 'model'), may hold values from -4 to 4
- slope_norm: bfloat16 [8, 1024], P('replica'), may hold values from -8 to 8
- param_query: float32 [1024, 1024], P('replica', 'model'), may hold values from -0.25 to 0.25
- param_key: float32 [1024, 1024], P('replica', 'model'), may hold values from -0.25 to 0.25
- param_value: float32 [1024, 1024], P('replica', 'model'), may hold values from -0.25 to 0.25
- param_mixed: float32 [1024, 1024], P('model', 'replica'), may hold values from -0.25 to 0.25
- param_norm: float32 [1024], P('replica'), may hold values from 0.25 to 1.75
- state_query: float32 [1024, 1024], P('replica', 'model'), may hold values from 0.0001953125 to 0.001953125
- state_key: float32 [1024, 1024], P('replica', 'model'), may hold values from 0.0001953125 to 0.001953125
- state_value: float32 [1024, 1024], P('replica', 'model'), may hold values from 0.0001953125 to 0.001953125
- state_mixed: float32 [1024, 1024], P('model', 'replica'), may hold values from 0.0001953125 to 0.001953125
- state_norm: float32 [1024], P('replica'), may hold values from 0.05 to 0.8
Outputs:
- half_query: bfloat16 [1024, 1024], P(None, 'model')
- half_key: bfloat16 [1024, 1024], P(None, 'model')
- half_value: bfloat16 [1024, 1024], P(None, 'model')
- half_mixed: bfloat16 [1024, 1024], P('model')
- half_norm: bfloat16 [1024], replicated
- next_query: float32 [1024, 1024], P('replica', 'model')
- next_key: float32 [1024, 1024], P('replica', 'model')
- next_value: float32 [1024, 1024], P('replica', 'model')
- next_mixed: float32 [1024, 1024], P('model', 'replica')
- next_norm: float32 [1024], P('replica')
- state_new_query: float32 [1024, 1024], P('replica', 'model')
- state_new_key: float32 [1024, 1024], P('replica', 'model')
- state_new_value: float32 [1024, 1024], P('replica', 'model')
- state_new_mixed: float32 [1024, 1024], P('model', 'replica')
- state_new_norm: float32 [1024], P('replica')
The draws below stay inside these ranges and needn't reach their ends.
All inputs are finite; a program needn't handle non-finite values.
Results may differ from the reference program's by a relative error of at most 0.001.
Values may be sent and summed in bfloat16 or wider, within the bound.
A program may use at most 64 MiB of HBM per device.

```python
import jax
import jax.numpy as jnp
from jax import lax

WIDTH = 1024
ATTN = 1024
REPLICAS = 8


def strengthened(array, key, source, target, shards_of, factor):
    owner, partner = [(jnp.arange(array.shape[dim]) // (array.shape[dim] // shards_of)).reshape([-1 if axis == dim else 1 for axis in range(array.ndim)]) for dim in (source, target)]
    chosen = jax.random.permutation(key, shards_of)[partner]
    strong = (owner == chosen) | (owner == (partner + shards_of // 2) % shards_of)
    return jnp.where(strong, factor * array, array)


def steps_of(own_key, shape, split, low, top_value):
    def one(position, parts):
        draws = jax.random.uniform(jax.random.fold_in(jax.random.fold_in(own_key, 6), position), (parts,), jnp.float32, low / len(split), top_value / len(split))
        return jnp.repeat(jnp.exp(draws), shape[position] // parts).reshape((-1,) + (1,) * (len(shape) - position - 1))

    factor_of = one(*split[0])
    for cut in split[1:]:
        factor_of = factor_of * one(*cut)
    return factor_of


def gaussian_with(stream_key, dims, deviation, reach, pieces, heavy, dtype=jnp.bfloat16):
    drawn = deviation * jax.random.normal(stream_key, dims, jnp.float32)
    if pieces:
        drawn = drawn * steps_of(stream_key, dims, pieces, -0.22, 0.18)
    return jnp.clip(strengthened(drawn, jax.random.fold_in(stream_key, 3), *heavy), -reach, reach).astype(dtype)


def setup_inputs(seed: int = 0) -> dict:
    streams_of = jax.random.split(jax.random.key(seed), 16)
    return {
        "slope_query": gaussian_with(streams_of[0], (REPLICAS, WIDTH, ATTN), 0.5, 4.0, ((0, 8), (2, 4)), (0, 1, 8, 2.0)),
        "slope_key": gaussian_with(streams_of[1], (REPLICAS, WIDTH, ATTN), 0.5, 4.0, ((0, 8), (2, 4)), (0, 1, 8, 2.0)),
        "slope_value": gaussian_with(streams_of[2], (REPLICAS, WIDTH, ATTN), 0.5, 4.0, ((0, 8), (2, 4)), (0, 1, 8, 2.0)),
        "slope_mixed": gaussian_with(streams_of[3], (REPLICAS, ATTN, WIDTH), 0.5, 4.0, ((0, 8), (1, 4)), (0, 2, 8, 2.0)),
        "slope_norm": gaussian_with(streams_of[4], (REPLICAS, WIDTH), 1.0, 8.0, ((0, 8),), (0, 1, 8, 2.0)),
        "param_query": gaussian_with(streams_of[5], (WIDTH, ATTN), WIDTH ** -0.5, 0.25, ((0, 8), (1, 4)), (1, 0, 8, 2.0), jnp.float32),
        "param_key": gaussian_with(streams_of[6], (WIDTH, ATTN), WIDTH ** -0.5, 0.25, ((0, 8), (1, 4)), (1, 0, 8, 2.0), jnp.float32),
        "param_value": gaussian_with(streams_of[7], (WIDTH, ATTN), WIDTH ** -0.5, 0.25, ((0, 8), (1, 4)), (1, 0, 8, 2.0), jnp.float32),
        "param_mixed": gaussian_with(streams_of[8], (ATTN, WIDTH), ATTN ** -0.5, 0.25, ((0, 4), (1, 8)), (0, 1, 8, 2.0), jnp.float32),
        "param_norm": jnp.clip(1.0 + 0.15 * jax.random.normal(streams_of[9], (WIDTH,), jnp.float32), 0.25, 1.75),
        "state_query": jnp.clip(0.0001953125 + 0.0017578125 * jax.random.uniform(streams_of[10], (WIDTH, ATTN), jnp.float32) ** steps_of(streams_of[10], (WIDTH, ATTN), ((0, 8), (1, 4)), -0.2, 0.2), 0.0001953125, 0.001953125),
        "state_key": jnp.clip(0.0001953125 + 0.0017578125 * jax.random.uniform(streams_of[11], (WIDTH, ATTN), jnp.float32) ** steps_of(streams_of[11], (WIDTH, ATTN), ((0, 8), (1, 4)), -0.2, 0.2), 0.0001953125, 0.001953125),
        "state_value": jnp.clip(0.0001953125 + 0.0017578125 * jax.random.uniform(streams_of[12], (WIDTH, ATTN), jnp.float32) ** steps_of(streams_of[12], (WIDTH, ATTN), ((0, 8), (1, 4)), -0.2, 0.2), 0.0001953125, 0.001953125),
        "state_mixed": jnp.clip(0.0001953125 + 0.0017578125 * jax.random.uniform(streams_of[13], (ATTN, WIDTH), jnp.float32) ** steps_of(streams_of[13], (ATTN, WIDTH), ((0, 4), (1, 8)), -0.2, 0.2), 0.0001953125, 0.001953125),
        "state_norm": jnp.clip(0.05 + 0.75 * jax.random.uniform(streams_of[14], (WIDTH,), jnp.float32) ** steps_of(streams_of[14], (WIDTH,), ((0, 8),), -0.2, 0.2), 0.05, 0.8),
    }


learn_rate = 0.025
hold_rate = 0.7

def reference(slope_query, slope_key, slope_value, slope_mixed, slope_norm, param_query, param_key, param_value, param_mixed, param_norm, state_query, state_key, state_value, state_mixed, state_norm):
    mean_query = lax.optimization_barrier(jnp.sum(slope_query.astype(jnp.float32), axis=0)) * REPLICAS ** (-0.5)
    mean_key = lax.optimization_barrier(jnp.sum(slope_key.astype(jnp.float32), axis=0)) * REPLICAS ** (-0.5)
    mean_value = lax.optimization_barrier(jnp.sum(slope_value.astype(jnp.float32), axis=0)) * REPLICAS ** (-0.5)
    mean_mixed = lax.optimization_barrier(jnp.sum(slope_mixed.astype(jnp.float32), axis=0)) * REPLICAS ** (-0.5)
    mean_norm = lax.optimization_barrier(jnp.sum(slope_norm.astype(jnp.float32), axis=0)) * REPLICAS ** (-0.5)
    ratio_query = jnp.sqrt(lax.optimization_barrier(jnp.sum(param_query * param_query, axis=1, keepdims=True))) * lax.rsqrt(lax.optimization_barrier(jnp.sum(mean_query * mean_query, axis=1, keepdims=True)) + 1e-06)
    mean_query = mean_query * ratio_query
    ratio_key = jnp.sqrt(lax.optimization_barrier(jnp.sum(param_key * param_key, axis=1, keepdims=True))) * lax.rsqrt(lax.optimization_barrier(jnp.sum(mean_key * mean_key, axis=1, keepdims=True)) + 1e-06)
    mean_key = mean_key * ratio_key
    ratio_value = jnp.sqrt(lax.optimization_barrier(jnp.sum(param_value * param_value, axis=1, keepdims=True))) * lax.rsqrt(lax.optimization_barrier(jnp.sum(mean_value * mean_value, axis=1, keepdims=True)) + 1e-06)
    mean_value = mean_value * ratio_value
    ratio_mixed = jnp.sqrt(lax.optimization_barrier(jnp.sum(param_mixed * param_mixed, axis=0, keepdims=True))) * lax.rsqrt(lax.optimization_barrier(jnp.sum(mean_mixed * mean_mixed, axis=0, keepdims=True)) + 1e-06)
    mean_mixed = mean_mixed * ratio_mixed
    state_new_query = hold_rate * state_query + (1.0 - hold_rate) * mean_query * mean_query
    next_query = param_query - learn_rate * mean_query * lax.rsqrt(state_new_query + 1e-06)
    state_new_key = hold_rate * state_key + (1.0 - hold_rate) * mean_key * mean_key
    next_key = param_key - learn_rate * mean_key * lax.rsqrt(state_new_key + 1e-06)
    state_new_value = hold_rate * state_value + (1.0 - hold_rate) * mean_value * mean_value
    next_value = param_value - learn_rate * mean_value * lax.rsqrt(state_new_value + 1e-06)
    state_new_mixed = hold_rate * state_mixed + (1.0 - hold_rate) * mean_mixed * mean_mixed
    next_mixed = param_mixed - learn_rate * mean_mixed * lax.rsqrt(state_new_mixed + 1e-06)
    state_new_norm = hold_rate * state_norm + (1.0 - hold_rate) * mean_norm * mean_norm
    next_norm = param_norm - learn_rate * mean_norm * lax.rsqrt(state_new_norm + 1e-06)
    half_query = next_query.astype(jnp.bfloat16)
    half_key = next_key.astype(jnp.bfloat16)
    half_value = next_value.astype(jnp.bfloat16)
    half_mixed = next_mixed.astype(jnp.bfloat16)
    half_norm = next_norm.astype(jnp.bfloat16)
    return (half_query, half_key, half_value, half_mixed, half_norm, next_query, next_key, next_value, next_mixed, next_norm, state_new_query, state_new_key, state_new_value, state_new_mixed, state_new_norm)
```

```python
import functools

import jax
import jax.numpy as jnp
from jax import lax
from jax.experimental import pallas as pl
from jax.experimental.pallas import tpu as pltpu
from jax.sharding import PartitionSpec as P

learn_rate = 0.025
hold_rate = 0.7
MESH = pl.DeviceIdType.MESH
LANES = 128
INNER = 2


def updated(param, mean, state):
    state_new = hold_rate * state + (1.0 - hold_rate) * mean * mean
    return param - learn_rate * mean * lax.rsqrt(state_new + 1e-06), state_new


def kernel(n, models, *refs):
    slopes, slope_norm = refs[0:4], refs[4]
    params, param_norm = refs[5:9], refs[9]
    states, state_norm = refs[10:14], refs[14]
    halves, half_norm = refs[15:19], refs[19]
    nexts, next_norm = refs[20:24], refs[24]
    state_news, state_new_norm = refs[25:29], refs[29]
    pair, ups, downs, totals = refs[30:34], refs[34:38], refs[38:42], refs[42:46]
    (
        own_sizes, mean_sizes, vector, parts,
        pair_send, pair_recv, up_send, up_recv, down_send, down_recv,
        give_up_send, give_up_recv, give_down_send, give_down_recv, give_pair_send, give_pair_recv,
        own_send, own_recv, mean_send, mean_recv,
        parts_send, parts_recv, norm_send, norm_recv,
    ) = refs[46:]
    outer = n // INNER
    rate = n ** (-0.5)
    me = lax.axis_index("replica")
    here = lax.axis_index("model")
    z, y = me // INNER, me % INNER
    width = param_norm.shape[1]
    partner = {"replica": z * INNER + (1 - y)}
    above = {"replica": lax.rem(me + INNER, n)}
    below = {"replica": lax.rem(me + n - INNER, n)}

    def block(m, ref, b):
        if m < 3:
            rows = params[m].shape[0]
            return ref.at[pl.ds(pl.multiple_of(b * rows, rows), rows), :]
        columns = params[m].shape[1]
        return ref.at[:, pl.ds(pl.multiple_of(b * columns, columns), columns)]

    def raw(m, b):
        return block(m, slopes[m].at[0], b)

    def remote(src, dst, send_sem, recv_sem, device):
        return pltpu.make_async_remote_copy(
            src_ref=src, dst_ref=dst, send_sem=send_sem, recv_sem=recv_sem,
            device_id=device, device_id_type=MESH,
        )

    def turn(i):
        return jnp.where(z < outer // 2, outer - 1 - i, i)

    def pair_copy(m, d):
        return remote(raw(m, d * INNER + (1 - y)), pair[m].at[d], pair_send.at[m, d], pair_recv.at[m, d], partner)

    def up_copy(m, d):
        return remote(ups[m].at[d], ups[m].at[d], up_send.at[m, d], up_recv.at[m, d], above)

    def down_copy(m, d):
        return remote(downs[m].at[d], downs[m].at[d], down_send.at[m, d], down_recv.at[m, d], below)

    def give_up(m, s):
        place = block(m, halves[m], s * INNER + y)
        return remote(place, place, give_up_send.at[m, s], give_up_recv.at[m, s], above)

    def give_down(m, s):
        place = block(m, halves[m], s * INNER + y)
        return remote(place, place, give_down_send.at[m, s], give_down_recv.at[m, s], below)

    def give_pair(m, s, side):
        place = block(m, halves[m], s * INNER + side)
        return remote(place, place, give_pair_send.at[m, s], give_pair_recv.at[m, s], partner)

    def own_copy(k):
        peer = lax.rem(here + k, models)
        return peer, remote(own_sizes.at[here], own_sizes.at[here], own_send.at[k], own_recv.at[here], {"model": peer})

    def mean_copy(m, k):
        peer = lax.rem(here + k, models)
        place = mean_sizes.at[m, here]
        return peer, remote(place, place, mean_send.at[m, k], mean_recv.at[m, here], {"model": peer})

    def parts_copy(k):
        peer = lax.rem(me + k, n)
        src = vector.at[:, pl.ds(pl.multiple_of(peer * width, width), width)]
        return peer, remote(src, parts.at[me], parts_send.at[k], parts_recv.at[me], {"replica": peer})

    def norm_copy(k):
        peer = lax.rem(me + k, n)
        return peer, remote(half_norm.at[me], half_norm.at[me], norm_send.at[k], norm_recv.at[me], {"replica": peer})

    def local_sum(m, d):
        return raw(m, d * INNER + y)[...].astype(jnp.float32) + pair[m][d].astype(jnp.float32)

    def sizes(m, value):
        square = value * value
        if m < 3:
            rows = square.shape[0]
            column = jnp.sum(square, axis=1, keepdims=True)
            return jnp.broadcast_to(column, (rows, LANES)).T[0:8]
        return jnp.broadcast_to(jnp.sum(square, axis=0, keepdims=True), (8, square.shape[1]))

    def send_sums(m):
        for i in range(outer):
            d = turn(i)
            pair_copy(m, d).wait_recv()

            @pl.when(d > z)
            def _():
                @pl.when(z > 0)
                def _():
                    up_copy(m, d).wait_recv()
                    ups[m][d] = ups[m][d] + local_sum(m, d)

                @pl.when(z == 0)
                def _():
                    ups[m][d] = local_sum(m, d)

                up_copy(m, d).start()

            @pl.when(d < z)
            def _():
                @pl.when(z < outer - 1)
                def _():
                    down_copy(m, d).wait_recv()
                    downs[m][d] = downs[m][d] + local_sum(m, d)

                @pl.when(z == outer - 1)
                def _():
                    downs[m][d] = local_sum(m, d)

                down_copy(m, d).start()

    def finish_sum(m):
        totals[m][...] = local_sum(m, z)

        @pl.when(z > 0)
        def _():
            up_copy(m, z).wait_recv()
            totals[m][...] += ups[m][z]

        @pl.when(z < outer - 1)
        def _():
            down_copy(m, z).wait_recv()
            totals[m][...] += downs[m][z]

        mean = totals[m][...] * rate
        totals[m][...] = mean
        mean_sizes[m, here] = sizes(m, mean)
        for k in range(1, models):
            mean_copy(m, k)[1].start()

    def update(m):
        for k in range(1, models):
            peer = lax.rem(here + k, models)
            place = mean_sizes.at[m, peer]
            remote(place, place, mean_send.at[m, k], mean_recv.at[m, peer], {"model": peer}).wait_recv()
        own = own_sizes[0, m]
        size = mean_sizes[m, 0]
        for k in range(1, models):
            own = own + own_sizes[k, m]
            size = size + mean_sizes[m, k]
        ratio = (jnp.sqrt(own) * lax.rsqrt(size + 1e-06))[0:1]
        shape = params[m].shape
        if m < 3:
            tile = jnp.broadcast_to(ratio, (LANES, shape[0])).T
            ratio = jnp.concatenate([tile] * (shape[1] // LANES), axis=1)
        next_value, state_new = updated(params[m][...], totals[m][...] * ratio, states[m][...])
        nexts[m][...] = next_value
        state_news[m][...] = state_new
        block(m, halves[m], me)[...] = next_value.astype(jnp.bfloat16)

        @pl.when(z < outer - 1)
        def _():
            give_up(m, z).start()

        @pl.when(z > 0)
        def _():
            give_down(m, z).start()

        give_pair(m, z, y).start()

    def relay(m):
        for k in range(1, outer):
            @pl.when(z >= k)
            def _():
                s = z - k
                give_up(m, s).wait_recv()

                @pl.when(z < outer - 1)
                def _():
                    give_up(m, s).start()

                give_pair(m, s, y).start()

            @pl.when(z + k < outer)
            def _():
                s = z + k
                give_down(m, s).wait_recv()

                @pl.when(z > 0)
                def _():
                    give_down(m, s).start()

                give_pair(m, s, y).start()

    def close(m):
        for s in range(outer):
            give_pair(m, s, 1 - y).wait_recv()
        for s in range(outer):
            pair_copy(m, s).wait_send()
            give_pair(m, s, y).wait_send()

            @pl.when(s > z)
            def _():
                up_copy(m, s).wait_send()

            @pl.when(s < z)
            def _():
                down_copy(m, s).wait_send()

            @pl.when(jnp.logical_and(s <= z, z < outer - 1))
            def _():
                give_up(m, s).wait_send()

            @pl.when(jnp.logical_and(s >= z, z > 0))
            def _():
                give_down(m, s).wait_send()

        for k in range(1, models):
            mean_copy(m, k)[1].wait_send()

    def vector_update():
        for k in range(1, n):
            peer = lax.rem(me + k, n)
            remote(parts.at[peer], parts.at[peer], parts_send.at[k], parts_recv.at[peer], {"replica": peer}).wait_recv()
        mean = parts[0]
        for k in range(1, n):
            mean = mean + parts[k]
        next_value, state_new = updated(param_norm[...], mean * rate, state_norm[...])
        next_norm[...] = next_value
        state_new_norm[...] = state_new
        half_norm[me] = next_value
        for k in range(1, n):
            norm_copy(k)[1].start()

    barrier = pltpu.get_barrier_semaphore()
    for k in range(1, n):
        pl.semaphore_signal(barrier, inc=1, device_id={"replica": lax.rem(me + k, n)}, device_id_type=MESH)
    for k in range(1, models):
        pl.semaphore_signal(barrier, inc=1, device_id={"model": lax.rem(here + k, models)}, device_id_type=MESH)
    for m in range(4):
        own_sizes[here, m] = sizes(m, params[m][...])
    vector[...] = slope_norm[...].astype(jnp.float32)
    parts[me] = vector[:, pl.ds(pl.multiple_of(me * width, width), width)]
    pl.semaphore_wait(barrier, n - 1 + models - 1)

    for m in range(4):
        for i in range(outer):
            pair_copy(m, turn(i)).start()
        if m == 0:
            for k in range(1, models):
                own_copy(k)[1].start()
            for k in range(1, n):
                parts_copy(k)[1].start()

    send_sums(0)
    vector_update()
    for k in range(1, models):
        peer = lax.rem(here + k, models)
        remote(own_sizes.at[peer], own_sizes.at[peer], own_send.at[k], own_recv.at[peer], {"model": peer}).wait_recv()
    send_sums(1)
    finish_sum(0)
    send_sums(2)
    update(0)
    finish_sum(1)
    send_sums(3)
    update(1)
    relay(0)
    finish_sum(2)
    update(2)
    relay(1)
    finish_sum(3)
    relay(2)
    update(3)
    relay(3)
    for m in range(4):
        close(m)
    for k in range(1, models):
        own_copy(k)[1].wait_send()
    for k in range(1, n):
        peer = lax.rem(me + k, n)
        remote(half_norm.at[peer], half_norm.at[peer], norm_send.at[k], norm_recv.at[peer], {"replica": peer}).wait_recv()
        parts_copy(k)[1].wait_send()
        norm_copy(k)[1].wait_send()


def fused(n, models, *args):
    slopes, params, states = args[0:5], args[5:10], args[10:15]
    outer = n // INNER
    width = params[4].shape[0]
    row = lambda a: a.reshape(1, width)
    shapes = [p.shape for p in params[0:4]]
    f32 = lambda s: jax.ShapeDtypeStruct(s, jnp.float32)
    out_shape = (
        [jax.ShapeDtypeStruct(s.shape[1:], jnp.bfloat16) for s in slopes[0:4]]
        + [f32((n, 1, width))]
        + ([f32(s) for s in shapes] + [f32((1, width))]) * 2
    )
    dma = lambda *s: pltpu.SemaphoreType.DMA(s)
    scratch = (
        [pltpu.VMEM((outer,) + s, jnp.bfloat16) for s in shapes]
        + [pltpu.VMEM((outer,) + s, jnp.float32) for s in shapes] * 2
        + [pltpu.VMEM(s, jnp.float32) for s in shapes]
        + [
            pltpu.VMEM((models, 4, 8, shapes[0][0]), jnp.float32),
            pltpu.VMEM((4, models, 8, shapes[0][0]), jnp.float32),
            pltpu.VMEM(slopes[4].shape, jnp.float32),
            pltpu.VMEM((n, 1, width), jnp.float32),
        ]
        + [dma(4, outer)] * 12
        + [dma(models)] * 2
        + [dma(4, models)] * 2
        + [dma(n)] * 4
    )
    outs = pl.pallas_call(
        functools.partial(kernel, n, models),
        out_shape=out_shape,
        in_specs=[pl.BlockSpec(memory_space=pltpu.VMEM)] * 15,
        out_specs=[pl.BlockSpec(memory_space=pltpu.VMEM)] * 15,
        scratch_shapes=scratch,
        compiler_params=pltpu.CompilerParams(collective_id=0, has_side_effects=True),
    )(*slopes, *params[0:4], row(params[4]), *states[0:4], row(states[4]))
    outs = list(outs)
    outs[4] = outs[4].reshape(-1).astype(jnp.bfloat16)
    outs[9] = outs[9].reshape(-1)
    outs[14] = outs[14].reshape(-1)
    return tuple(outs)


def plain(*args):
    slopes, params, states = args[0:5], args[5:10], args[10:15]
    rate = lax.axis_size("replica") ** (-0.5)
    dims = (0, 0, 0, 1)
    means = [
        lax.psum_scatter(s[0].astype(jnp.float32), "replica", scatter_dimension=d, tiled=True) * rate
        for s, d in zip(slopes, dims)
    ]
    whole = lax.psum(slopes[4][0].astype(jnp.float32), "replica")
    width = params[4].shape[0]
    mean_norm = lax.dynamic_slice_in_dim(whole, lax.axis_index("replica") * width, width) * rate
    size = lambda a, d: jnp.sum(a * a, axis=1 - d, keepdims=True)
    own, got = lax.psum(
        ([size(p, d) for p, d in zip(params, dims)], [size(a, d) for a, d in zip(means, dims)]), "model"
    )
    means = [a * (jnp.sqrt(o) * lax.rsqrt(g + 1e-06)) for a, o, g in zip(means, own, got)] + [mean_norm]
    pairs = [updated(p, a, s) for p, a, s in zip(params, means, states)]
    halves = [
        lax.all_gather(v.astype(jnp.bfloat16), "replica", axis=d, tiled=True)
        for (v, _), d in zip(pairs, dims + (0,))
    ]
    return tuple(halves) + tuple(v for v, _ in pairs) + tuple(s for _, s in pairs)


def solution(mesh):
    n, models = mesh.shape["replica"], mesh.shape["model"]

    def local(*args):
        rows, columns, width = args[5].shape[0], args[8].shape[1], args[9].shape[0]
        aligned = rows % LANES == 0 and columns % LANES == 0 and width % LANES == 0
        if n % INNER == 0 and aligned and rows == columns:
            return fused(n, models, *args)
        return plain(*args)

    inner, turned = P("replica", "model"), P("model", "replica")
    slices = (P("replica", None, "model"),) * 3 + (P("replica", "model", None), P("replica", None))
    shares = (inner,) * 3 + (turned, P("replica"))
    return jax.shard_map(
        local,
        mesh=mesh,
        in_specs=slices + shares * 2,
        out_specs=(P(None, "model"),) * 3 + (P("model", None), P()) + shares * 2,
        check_vma=False,
    )
```

```python
import functools

import jax
import jax.numpy as jnp
from jax import lax
from jax.experimental import pallas as pl
from jax.experimental.pallas import tpu as pltpu
from jax.sharding import PartitionSpec as P

learn_rate = 0.025
hold_rate = 0.7
MESH = pl.DeviceIdType.MESH
LANES = 128
INNER = 2


def updated(param, mean, state):
    state_new = hold_rate * state + (1.0 - hold_rate) * mean * mean
    return param - learn_rate * mean * lax.rsqrt(state_new + 1e-06), state_new


def kernel(n, models, *refs):
    slopes_far, slope_norm = refs[0:4], refs[4]
    params_far, param_norm = refs[5:9], refs[9]
    states_far, state_norm = refs[10:14], refs[14]
    halves_far, half_norm = refs[15:19], refs[19]
    nexts_far, next_norm = refs[20:24], refs[24]
    state_news_far, state_new_norm = refs[25:29], refs[29]
    pair, ups, downs, totals = refs[30:34], refs[34:38], refs[38:42], refs[42:46]
    slopes, params, states = refs[46:50], refs[50:54], refs[54:58]
    halves, nexts, state_news = refs[58:62], refs[62:66], refs[66:70]
    (
        own_sizes, mean_sizes, vector, parts,
        pair_send, pair_recv, up_send, up_recv, down_send, down_recv,
        give_up_send, give_up_recv, give_down_send, give_down_recv, give_pair_send, give_pair_recv,
        own_send, own_recv, mean_send, mean_recv,
        parts_send, parts_recv, norm_send, norm_recv, near,
    ) = refs[70:]
    outer = n // INNER
    rate = n ** (-0.5)
    me = lax.axis_index("replica")
    here = lax.axis_index("model")
    z, y = me // INNER, me % INNER
    width = param_norm.shape[1]
    partner = {"replica": z * INNER + (1 - y)}
    above = {"replica": lax.rem(me + INNER, n)}
    below = {"replica": lax.rem(me + n - INNER, n)}

    def block(m, ref, b):
        if m < 3:
            rows = params[m].shape[0]
            return ref.at[pl.ds(pl.multiple_of(b * rows, rows), rows), :]
        columns = params[m].shape[1]
        return ref.at[:, pl.ds(pl.multiple_of(b * columns, columns), columns)]

    def raw(m, b):
        return block(m, slopes[m], b)

    def remote(src, dst, send_sem, recv_sem, device):
        return pltpu.make_async_remote_copy(
            src_ref=src, dst_ref=dst, send_sem=send_sem, recv_sem=recv_sem,
            device_id=device, device_id_type=MESH,
        )

    def turn(i):
        return jnp.where(z < outer // 2, outer - 1 - i, i)

    def pair_copy(m, d):
        return remote(raw(m, d * INNER + (1 - y)), pair[m].at[d], pair_send.at[m, d], pair_recv.at[m, d], partner)

    def up_copy(m, d):
        return remote(ups[m].at[d], ups[m].at[d], up_send.at[m, d], up_recv.at[m, d], above)

    def down_copy(m, d):
        return remote(downs[m].at[d], downs[m].at[d], down_send.at[m, d], down_recv.at[m, d], below)

    def give_up(m, s):
        place = block(m, halves[m], s * INNER + y)
        return remote(place, place, give_up_send.at[m, s], give_up_recv.at[m, s], above)

    def give_down(m, s):
        place = block(m, halves[m], s * INNER + y)
        return remote(place, place, give_down_send.at[m, s], give_down_recv.at[m, s], below)

    def give_pair(m, s, side):
        place = block(m, halves[m], s * INNER + side)
        return remote(place, place, give_pair_send.at[m, s], give_pair_recv.at[m, s], partner)

    def own_copy(k):
        peer = lax.rem(here + k, models)
        return peer, remote(own_sizes.at[here], own_sizes.at[here], own_send.at[k], own_recv.at[here], {"model": peer})

    def mean_copy(m, k):
        peer = lax.rem(here + k, models)
        place = mean_sizes.at[m, here]
        return peer, remote(place, place, mean_send.at[m, k], mean_recv.at[m, here], {"model": peer})

    def parts_copy(k):
        peer = lax.rem(me + k, n)
        src = vector.at[:, pl.ds(pl.multiple_of(peer * width, width), width)]
        return peer, remote(src, parts.at[me], parts_send.at[k], parts_recv.at[me], {"replica": peer})

    def norm_copy(k):
        peer = lax.rem(me + k, n)
        return peer, remote(half_norm.at[me], half_norm.at[me], norm_send.at[k], norm_recv.at[me], {"replica": peer})

    def load_slope(m):
        return pltpu.make_async_copy(slopes_far[m].at[0], slopes[m], near.at[0, m])

    def load_param(m):
        return pltpu.make_async_copy(params_far[m], params[m], near.at[1, m])

    def load_state(m):
        return pltpu.make_async_copy(states_far[m], states[m], near.at[2, m])

    def store_half(m):
        return pltpu.make_async_copy(halves[m], halves_far[m], near.at[3, m])

    def store_next(m):
        return pltpu.make_async_copy(nexts[m], nexts_far[m], near.at[4, m])

    def store_state(m):
        return pltpu.make_async_copy(state_news[m], state_news_far[m], near.at[5, m])

    def local_sum(m, d):
        return raw(m, d * INNER + y)[...].astype(jnp.float32) + pair[m][d].astype(jnp.float32)

    def sizes(m, value):
        square = value * value
        if m < 3:
            rows = square.shape[0]
            column = jnp.sum(square, axis=1, keepdims=True)
            return jnp.broadcast_to(column, (rows, LANES)).T[0:8]
        return jnp.broadcast_to(jnp.sum(square, axis=0, keepdims=True), (8, square.shape[1]))

    def send_sums(m):
        for i in range(outer):
            d = turn(i)
            pair_copy(m, d).wait_recv()

            @pl.when(d > z)
            def _():
                @pl.when(z > 0)
                def _():
                    up_copy(m, d).wait_recv()
                    ups[m][d] = ups[m][d] + local_sum(m, d)

                @pl.when(z == 0)
                def _():
                    ups[m][d] = local_sum(m, d)

                up_copy(m, d).start()

            @pl.when(d < z)
            def _():
                @pl.when(z < outer - 1)
                def _():
                    down_copy(m, d).wait_recv()
                    downs[m][d] = downs[m][d] + local_sum(m, d)

                @pl.when(z == outer - 1)
                def _():
                    downs[m][d] = local_sum(m, d)

                down_copy(m, d).start()

    def finish_sum(m):
        totals[m][...] = local_sum(m, z)

        @pl.when(z > 0)
        def _():
            up_copy(m, z).wait_recv()
            totals[m][...] += ups[m][z]

        @pl.when(z < outer - 1)
        def _():
            down_copy(m, z).wait_recv()
            totals[m][...] += downs[m][z]

        mean = totals[m][...] * rate
        totals[m][...] = mean
        mean_sizes[m, here] = sizes(m, mean)
        for k in range(1, models):
            mean_copy(m, k)[1].start()

    def update(m):
        for k in range(1, models):
            peer = lax.rem(here + k, models)
            place = mean_sizes.at[m, peer]
            remote(place, place, mean_send.at[m, k], mean_recv.at[m, peer], {"model": peer}).wait_recv()
        own = own_sizes[0, m]
        size = mean_sizes[m, 0]
        for k in range(1, models):
            own = own + own_sizes[k, m]
            size = size + mean_sizes[m, k]
        ratio = (jnp.sqrt(own) * lax.rsqrt(size + 1e-06))[0:1]
        shape = params[m].shape
        if m < 3:
            tile = jnp.broadcast_to(ratio, (LANES, shape[0])).T
            ratio = jnp.concatenate([tile] * (shape[1] // LANES), axis=1)
        next_value, state_new = updated(params[m][...], totals[m][...] * ratio, states[m][...])
        nexts[m][...] = next_value
        state_news[m][...] = state_new
        block(m, halves[m], me)[...] = next_value.astype(jnp.bfloat16)

        @pl.when(z < outer - 1)
        def _():
            give_up(m, z).start()

        @pl.when(z > 0)
        def _():
            give_down(m, z).start()

        give_pair(m, z, y).start()
        store_next(m).start()
        store_state(m).start()

    def relay(m):
        for k in range(1, outer):
            @pl.when(z >= k)
            def _():
                s = z - k
                give_up(m, s).wait_recv()

                @pl.when(z < outer - 1)
                def _():
                    give_up(m, s).start()

                give_pair(m, s, y).start()

            @pl.when(z + k < outer)
            def _():
                s = z + k
                give_down(m, s).wait_recv()

                @pl.when(z > 0)
                def _():
                    give_down(m, s).start()

                give_pair(m, s, y).start()

    def close(m):
        for s in range(outer):
            give_pair(m, s, 1 - y).wait_recv()
        store_half(m).start()
        for s in range(outer):
            pair_copy(m, s).wait_send()
            give_pair(m, s, y).wait_send()

            @pl.when(s > z)
            def _():
                up_copy(m, s).wait_send()

            @pl.when(s < z)
            def _():
                down_copy(m, s).wait_send()

            @pl.when(jnp.logical_and(s <= z, z < outer - 1))
            def _():
                give_up(m, s).wait_send()

            @pl.when(jnp.logical_and(s >= z, z > 0))
            def _():
                give_down(m, s).wait_send()

        for k in range(1, models):
            mean_copy(m, k)[1].wait_send()

    def vector_update():
        for k in range(1, n):
            peer = lax.rem(me + k, n)
            remote(parts.at[peer], parts.at[peer], parts_send.at[k], parts_recv.at[peer], {"replica": peer}).wait_recv()
        mean = parts[0]
        for k in range(1, n):
            mean = mean + parts[k]
        next_value, state_new = updated(param_norm[...], mean * rate, state_norm[...])
        next_norm[...] = next_value
        state_new_norm[...] = state_new
        half_norm[me] = next_value
        for k in range(1, n):
            norm_copy(k)[1].start()

    for load in (load_slope, load_param, load_state):
        for m in range(4):
            load(m).start()
    barrier = pltpu.get_barrier_semaphore()
    for k in range(1, n):
        pl.semaphore_signal(barrier, inc=1, device_id={"replica": lax.rem(me + k, n)}, device_id_type=MESH)
    for k in range(1, models):
        pl.semaphore_signal(barrier, inc=1, device_id={"model": lax.rem(here + k, models)}, device_id_type=MESH)
    vector[...] = slope_norm[...].astype(jnp.float32)
    parts[me] = vector[:, pl.ds(pl.multiple_of(me * width, width), width)]
    pl.semaphore_wait(barrier, n - 1 + models - 1)

    for m in range(4):
        load_slope(m).wait()
        for i in range(outer):
            pair_copy(m, turn(i)).start()
    for k in range(1, n):
        parts_copy(k)[1].start()
    for m in range(4):
        load_param(m).wait()
        load_state(m).wait()
        own_sizes[here, m] = sizes(m, params[m][...])
    for k in range(1, models):
        own_copy(k)[1].start()

    send_sums(0)
    vector_update()
    for k in range(1, models):
        peer = lax.rem(here + k, models)
        remote(own_sizes.at[peer], own_sizes.at[peer], own_send.at[k], own_recv.at[peer], {"model": peer}).wait_recv()
    inside = jnp.logical_and(z > 0, z < outer - 1)

    @pl.when(inside)
    def _():
        finish_sum(0)
        send_sums(1)
        update(0)
        finish_sum(1)
        send_sums(2)
        update(1)
        finish_sum(2)
        relay(0)
        send_sums(3)
        update(2)
        finish_sum(3)
        relay(1)
        update(3)
        relay(2)
        relay(3)

    @pl.when(jnp.logical_not(inside))
    def _():
        send_sums(1)
        finish_sum(0)
        send_sums(2)
        update(0)
        finish_sum(1)
        send_sums(3)
        update(1)
        finish_sum(2)
        relay(0)
        update(2)
        finish_sum(3)
        relay(1)
        update(3)
        relay(2)
        relay(3)

    for m in range(4):
        close(m)
    for k in range(1, models):
        own_copy(k)[1].wait_send()
    for k in range(1, n):
        peer = lax.rem(me + k, n)
        remote(half_norm.at[peer], half_norm.at[peer], norm_send.at[k], norm_recv.at[peer], {"replica": peer}).wait_recv()
        parts_copy(k)[1].wait_send()
        norm_copy(k)[1].wait_send()
    for m in range(4):
        store_next(m).wait()
        store_state(m).wait()
        store_half(m).wait()


def place_kernel(count, *refs):
    sources, targets, held = refs[0:count], refs[count : 2 * count], refs[2 * count : 3 * count]
    come, go = refs[3 * count :]
    into = [pltpu.make_async_copy(a, b, come.at[i]) for i, (a, b) in enumerate(zip(sources, held))]
    out = [pltpu.make_async_copy(a, b, go.at[i]) for i, (a, b) in enumerate(zip(held, targets))]
    for copy in into:
        copy.start()
    for i in range(count):
        into[i].wait()
        out[i].start()
    for copy in out:
        copy.wait()


def placed(arrays):
    count = len(arrays)
    anywhere = [pl.BlockSpec(memory_space=pl.ANY)] * count
    return pl.pallas_call(
        functools.partial(place_kernel, count),
        out_shape=[jax.ShapeDtypeStruct(a.shape, a.dtype) for a in arrays],
        in_specs=anywhere,
        out_specs=anywhere,
        scratch_shapes=[pltpu.VMEM(a.shape, a.dtype) for a in arrays] + [pltpu.SemaphoreType.DMA((count,))] * 2,
    )(*arrays)


def fused(n, models, *args):
    slopes, params, states = args[0:5], args[5:10], args[10:15]
    outer = n // INNER
    width = params[4].shape[0]
    row = lambda a: a.reshape(1, width)
    shapes = [p.shape for p in params[0:4]]
    f32 = lambda s: jax.ShapeDtypeStruct(s, jnp.float32)
    out_shape = (
        [jax.ShapeDtypeStruct(s.shape[1:], jnp.bfloat16) for s in slopes[0:4]]
        + [f32((n, 1, width))]
        + ([f32(s) for s in shapes] + [f32((1, width))]) * 2
    )
    dma = lambda *s: pltpu.SemaphoreType.DMA(s)
    scratch = (
        [pltpu.VMEM((outer,) + s, jnp.bfloat16) for s in shapes]
        + [pltpu.VMEM((outer,) + s, jnp.float32) for s in shapes] * 2
        + [pltpu.VMEM(s, jnp.float32) for s in shapes]
        + [pltpu.VMEM(s.shape[1:], jnp.bfloat16) for s in slopes[0:4]]
        + [pltpu.VMEM(s, jnp.float32) for s in shapes] * 2
        + [pltpu.VMEM(s.shape[1:], jnp.bfloat16) for s in slopes[0:4]]
        + [pltpu.VMEM(s, jnp.float32) for s in shapes] * 2
        + [
            pltpu.VMEM((models, 4, 8, shapes[0][0]), jnp.float32),
            pltpu.VMEM((4, models, 8, shapes[0][0]), jnp.float32),
            pltpu.VMEM(slopes[4].shape, jnp.float32),
            pltpu.VMEM((n, 1, width), jnp.float32),
        ]
        + [dma(4, outer)] * 12
        + [dma(models)] * 2
        + [dma(4, models)] * 2
        + [dma(n)] * 4
        + [dma(6, 4)]
    )
    specs = ([pl.BlockSpec(memory_space=pl.ANY)] * 4 + [pl.BlockSpec(memory_space=pltpu.VMEM)]) * 3
    outs = pl.pallas_call(
        functools.partial(kernel, n, models),
        out_shape=out_shape,
        in_specs=specs,
        out_specs=specs,
        scratch_shapes=scratch,
        compiler_params=pltpu.CompilerParams(collective_id=0, has_side_effects=True),
    )(*slopes, *params[0:4], row(params[4]), *states[0:4], row(states[4]))
    outs = list(outs)
    moved = [i for i in range(15) if i != 4]
    for i, a in zip(moved, placed([outs[i] for i in moved])):
        outs[i] = a
    outs[4] = outs[4].reshape(-1).astype(jnp.bfloat16)
    outs[9] = outs[9].reshape(-1)
    outs[14] = outs[14].reshape(-1)
    return tuple(outs)


def plain(*args):
    slopes, params, states = args[0:5], args[5:10], args[10:15]
    rate = lax.axis_size("replica") ** (-0.5)
    dims = (0, 0, 0, 1)
    means = [
        lax.psum_scatter(s[0].astype(jnp.float32), "replica", scatter_dimension=d, tiled=True) * rate
        for s, d in zip(slopes, dims)
    ]
    whole = lax.psum(slopes[4][0].astype(jnp.float32), "replica")
    width = params[4].shape[0]
    mean_norm = lax.dynamic_slice_in_dim(whole, lax.axis_index("replica") * width, width) * rate
    size = lambda a, d: jnp.sum(a * a, axis=1 - d, keepdims=True)
    own, got = lax.psum(
        ([size(p, d) for p, d in zip(params, dims)], [size(a, d) for a, d in zip(means, dims)]), "model"
    )
    means = [a * (jnp.sqrt(o) * lax.rsqrt(g + 1e-06)) for a, o, g in zip(means, own, got)] + [mean_norm]
    pairs = [updated(p, a, s) for p, a, s in zip(params, means, states)]
    halves = [
        lax.all_gather(v.astype(jnp.bfloat16), "replica", axis=d, tiled=True)
        for (v, _), d in zip(pairs, dims + (0,))
    ]
    return tuple(halves) + tuple(v for v, _ in pairs) + tuple(s for _, s in pairs)


def solution(mesh):
    n, models = mesh.shape["replica"], mesh.shape["model"]

    def local(*args):
        rows, columns, width = args[5].shape[0], args[8].shape[1], args[9].shape[0]
        aligned = rows % LANES == 0 and columns % LANES == 0 and width % LANES == 0
        if n % INNER == 0 and aligned and rows == columns:
            return fused(n, models, *args)
        return plain(*args)

    inner, turned = P("replica", "model"), P("model", "replica")
    slices = (P("replica", None, "model"),) * 3 + (P("replica", "model", None), P("replica", None))
    shares = (inner,) * 3 + (turned, P("replica"))
    return jax.shard_map(
        local,
        mesh=mesh,
        in_specs=slices + shares * 2,
        out_specs=(P(None, "model"),) * 3 + (P("model", None), P()) + shares * 2,
        check_vma=False,
    )
```

```python
import functools

import jax
import jax.numpy as jnp
from jax import lax
from jax.experimental import pallas as pl
from jax.experimental.pallas import tpu as pltpu
from jax.sharding import PartitionSpec as P

learn_rate = 0.025
hold_rate = 0.7
MESH = pl.DeviceIdType.MESH
LANES = 128
INNER = 2


def updated(param, mean, state):
    state_new = hold_rate * state + (1.0 - hold_rate) * mean * mean
    return param - learn_rate * mean * lax.rsqrt(state_new + 1e-06), state_new


def kernel(n, models, *refs):
    slopes_far, slope_norm = refs[0:4], refs[4]
    params_far, param_norm = refs[5:9], refs[9]
    states_far, state_norm = refs[10:14], refs[14]
    halves_far, half_norm = refs[15:19], refs[19]
    nexts_far, next_norm = refs[20:24], refs[24]
    state_news_far, state_new_norm = refs[25:29], refs[29]
    pair, ups, downs, totals = refs[30:34], refs[34:38], refs[38:42], refs[42:46]
    slopes, params, states = refs[46:50], refs[50:54], refs[54:58]
    halves, nexts, state_news = refs[58:62], refs[62:66], refs[66:70]
    (
        own_sizes, mean_sizes, vector, parts,
        pair_send, pair_recv, up_send, up_recv, down_send, down_recv,
        give_up_send, give_up_recv, give_down_send, give_down_recv, give_pair_send, give_pair_recv,
        own_send, own_recv, mean_send, mean_recv,
        parts_send, parts_recv, norm_send, norm_recv, near,
    ) = refs[70:]
    outer = n // INNER
    rate = n ** (-0.5)
    me = lax.axis_index("replica")
    here = lax.axis_index("model")
    z, y = me // INNER, me % INNER
    width = param_norm.shape[1]
    partner = {"replica": z * INNER + (1 - y)}
    above = {"replica": lax.rem(me + INNER, n)}
    below = {"replica": lax.rem(me + n - INNER, n)}

    def block(m, ref, b):
        if m < 3:
            rows = params[m].shape[0]
            return ref.at[pl.ds(pl.multiple_of(b * rows, rows), rows), :]
        columns = params[m].shape[1]
        return ref.at[:, pl.ds(pl.multiple_of(b * columns, columns), columns)]

    def raw(m, b):
        return block(m, slopes[m], b)

    def remote(src, dst, send_sem, recv_sem, device):
        return pltpu.make_async_remote_copy(
            src_ref=src, dst_ref=dst, send_sem=send_sem, recv_sem=recv_sem,
            device_id=device, device_id_type=MESH,
        )

    def turn(i):
        return jnp.where(z < outer // 2, outer - 1 - i, i)

    def pair_copy(m, d):
        return remote(raw(m, d * INNER + (1 - y)), pair[m].at[d], pair_send.at[m, d], pair_recv.at[m, d], partner)

    def up_copy(m, d):
        return remote(ups[m].at[d], ups[m].at[d], up_send.at[m, d], up_recv.at[m, d], above)

    def down_copy(m, d):
        return remote(downs[m].at[d], downs[m].at[d], down_send.at[m, d], down_recv.at[m, d], below)

    def give_up(m, s):
        place = block(m, halves[m], s * INNER + y)
        return remote(place, place, give_up_send.at[m, s], give_up_recv.at[m, s], above)

    def give_down(m, s):
        place = block(m, halves[m], s * INNER + y)
        return remote(place, place, give_down_send.at[m, s], give_down_recv.at[m, s], below)

    def give_pair(m, s, side):
        place = block(m, halves[m], s * INNER + side)
        return remote(place, place, give_pair_send.at[m, s], give_pair_recv.at[m, s], partner)

    def own_copy(k):
        peer = lax.rem(here + k, models)
        return peer, remote(own_sizes.at[here], own_sizes.at[here], own_send.at[k], own_recv.at[here], {"model": peer})

    def mean_copy(m, k):
        peer = lax.rem(here + k, models)
        place = mean_sizes.at[m, here]
        return peer, remote(place, place, mean_send.at[m, k], mean_recv.at[m, here], {"model": peer})

    def parts_copy(k):
        peer = lax.rem(me + k, n)
        src = vector.at[:, pl.ds(pl.multiple_of(peer * width, width), width)]
        return peer, remote(src, parts.at[me], parts_send.at[k], parts_recv.at[me], {"replica": peer})

    def norm_copy(k):
        peer = lax.rem(me + k, n)
        return peer, remote(half_norm.at[me], half_norm.at[me], norm_send.at[k], norm_recv.at[me], {"replica": peer})

    def load_slope(m):
        return pltpu.make_async_copy(slopes_far[m].at[0], slopes[m], near.at[0, m])

    def load_param(m):
        return pltpu.make_async_copy(params_far[m], params[m], near.at[1, m])

    def load_state(m):
        return pltpu.make_async_copy(states_far[m], states[m], near.at[2, m])

    def store_half(m):
        return pltpu.make_async_copy(halves[m], halves_far[m], near.at[3, m])

    def store_next(m):
        return pltpu.make_async_copy(nexts[m], nexts_far[m], near.at[4, m])

    def store_state(m):
        return pltpu.make_async_copy(state_news[m], state_news_far[m], near.at[5, m])

    def local_sum(m, d):
        return raw(m, d * INNER + y)[...].astype(jnp.float32) + pair[m][d].astype(jnp.float32)

    def sizes(m, value):
        square = value * value
        if m < 3:
            rows = square.shape[0]
            column = jnp.sum(square, axis=1, keepdims=True)
            return jnp.broadcast_to(column, (rows, LANES)).T[0:8]
        return jnp.broadcast_to(jnp.sum(square, axis=0, keepdims=True), (8, square.shape[1]))

    def send_sums(m):
        for i in range(outer):
            d = turn(i)
            pair_copy(m, d).wait_recv()

            @pl.when(d > z)
            def _():
                @pl.when(z > 0)
                def _():
                    up_copy(m, d).wait_recv()
                    ups[m][d] = ups[m][d] + local_sum(m, d)

                @pl.when(z == 0)
                def _():
                    ups[m][d] = local_sum(m, d)

                up_copy(m, d).start()

            @pl.when(d < z)
            def _():
                @pl.when(z < outer - 1)
                def _():
                    down_copy(m, d).wait_recv()
                    downs[m][d] = downs[m][d] + local_sum(m, d)

                @pl.when(z == outer - 1)
                def _():
                    downs[m][d] = local_sum(m, d)

                down_copy(m, d).start()

    def finish_sum(m):
        totals[m][...] = local_sum(m, z)

        @pl.when(z > 0)
        def _():
            up_copy(m, z).wait_recv()
            totals[m][...] += ups[m][z]

        @pl.when(z < outer - 1)
        def _():
            down_copy(m, z).wait_recv()
            totals[m][...] += downs[m][z]

        mean = totals[m][...] * rate
        totals[m][...] = mean
        mean_sizes[m, here] = sizes(m, mean)
        for k in range(1, models):
            mean_copy(m, k)[1].start()

    def update(m):
        for k in range(1, models):
            peer = lax.rem(here + k, models)
            place = mean_sizes.at[m, peer]
            remote(place, place, mean_send.at[m, k], mean_recv.at[m, peer], {"model": peer}).wait_recv()
        own = own_sizes[0, m]
        size = mean_sizes[m, 0]
        for k in range(1, models):
            own = own + own_sizes[k, m]
            size = size + mean_sizes[m, k]
        ratio = (jnp.sqrt(own) * lax.rsqrt(size + 1e-06))[0:1]
        shape = params[m].shape
        if m < 3:
            tile = jnp.broadcast_to(ratio, (LANES, shape[0])).T
            ratio = jnp.concatenate([tile] * (shape[1] // LANES), axis=1)
        next_value, state_new = updated(params[m][...], totals[m][...] * ratio, states[m][...])
        nexts[m][...] = next_value
        state_news[m][...] = state_new
        block(m, halves[m], me)[...] = next_value.astype(jnp.bfloat16)

        @pl.when(z < outer - 1)
        def _():
            give_up(m, z).start()

        @pl.when(z > 0)
        def _():
            give_down(m, z).start()

        give_pair(m, z, y).start()
        store_next(m).start()
        store_state(m).start()

    def relay(m):
        for k in range(1, outer):
            @pl.when(z >= k)
            def _():
                s = z - k
                give_up(m, s).wait_recv()

                @pl.when(z < outer - 1)
                def _():
                    give_up(m, s).start()

                give_pair(m, s, y).start()

            @pl.when(z + k < outer)
            def _():
                s = z + k
                give_down(m, s).wait_recv()

                @pl.when(z > 0)
                def _():
                    give_down(m, s).start()

                give_pair(m, s, y).start()

    def close(m):
        for s in range(outer):
            give_pair(m, s, 1 - y).wait_recv()
        store_half(m).start()
        for s in range(outer):
            pair_copy(m, s).wait_send()
            give_pair(m, s, y).wait_send()

            @pl.when(s > z)
            def _():
                up_copy(m, s).wait_send()

            @pl.when(s < z)
            def _():
                down_copy(m, s).wait_send()

            @pl.when(jnp.logical_and(s <= z, z < outer - 1))
            def _():
                give_up(m, s).wait_send()

            @pl.when(jnp.logical_and(s >= z, z > 0))
            def _():
                give_down(m, s).wait_send()

        for k in range(1, models):
            mean_copy(m, k)[1].wait_send()

    def vector_update():
        for k in range(1, n):
            peer = lax.rem(me + k, n)
            remote(parts.at[peer], parts.at[peer], parts_send.at[k], parts_recv.at[peer], {"replica": peer}).wait_recv()
        mean = parts[0]
        for k in range(1, n):
            mean = mean + parts[k]
        next_value, state_new = updated(param_norm[...], mean * rate, state_norm[...])
        next_norm[...] = next_value
        state_new_norm[...] = state_new
        half_norm[me] = next_value
        for k in range(1, n):
            norm_copy(k)[1].start()

    for load in (load_slope, load_param, load_state):
        for m in range(4):
            load(m).start()
    barrier = pltpu.get_barrier_semaphore()
    for k in range(1, n):
        pl.semaphore_signal(barrier, inc=1, device_id={"replica": lax.rem(me + k, n)}, device_id_type=MESH)
    for k in range(1, models):
        pl.semaphore_signal(barrier, inc=1, device_id={"model": lax.rem(here + k, models)}, device_id_type=MESH)
    vector[...] = slope_norm[...].astype(jnp.float32)
    parts[me] = vector[:, pl.ds(pl.multiple_of(me * width, width), width)]
    pl.semaphore_wait(barrier, n - 1 + models - 1)

    for m in range(4):
        load_slope(m).wait()
        for i in range(outer):
            pair_copy(m, turn(i)).start()
    for k in range(1, n):
        parts_copy(k)[1].start()
    for m in range(4):
        load_param(m).wait()
        load_state(m).wait()
        own_sizes[here, m] = sizes(m, params[m][...])
    for k in range(1, models):
        own_copy(k)[1].start()

    send_sums(0)
    vector_update()
    for k in range(1, models):
        peer = lax.rem(here + k, models)
        remote(own_sizes.at[peer], own_sizes.at[peer], own_send.at[k], own_recv.at[peer], {"model": peer}).wait_recv()
    inside = jnp.logical_and(z > 0, z < outer - 1)

    @pl.when(inside)
    def _():
        finish_sum(0)
        send_sums(1)
        update(0)
        finish_sum(1)
        send_sums(2)
        update(1)
        finish_sum(2)
        send_sums(3)
        update(2)
        relay(0)
        finish_sum(3)
        update(3)
        relay(1)
        relay(2)
        relay(3)

    @pl.when(jnp.logical_not(inside))
    def _():
        send_sums(1)
        finish_sum(0)
        send_sums(2)
        update(0)
        finish_sum(1)
        send_sums(3)
        update(1)
        finish_sum(2)
        update(2)
        relay(0)
        finish_sum(3)
        update(3)
        relay(1)
        relay(2)
        relay(3)

    for m in range(4):
        close(m)
    for k in range(1, models):
        own_copy(k)[1].wait_send()
    for k in range(1, n):
        peer = lax.rem(me + k, n)
        remote(half_norm.at[peer], half_norm.at[peer], norm_send.at[k], norm_recv.at[peer], {"replica": peer}).wait_recv()
        parts_copy(k)[1].wait_send()
        norm_copy(k)[1].wait_send()
    for m in range(4):
        store_next(m).wait()
        store_state(m).wait()
        store_half(m).wait()


def place_kernel(count, *refs):
    sources, targets, held = refs[0:count], refs[count : 2 * count], refs[2 * count : 3 * count]
    come, go = refs[3 * count :]
    into = [pltpu.make_async_copy(a, b, come.at[i]) for i, (a, b) in enumerate(zip(sources, held))]
    out = [pltpu.make_async_copy(a, b, go.at[i]) for i, (a, b) in enumerate(zip(held, targets))]
    for copy in into:
        copy.start()
    for i in range(count):
        into[i].wait()
        out[i].start()
    for copy in out:
        copy.wait()


def placed(arrays):
    count = len(arrays)
    anywhere = [pl.BlockSpec(memory_space=pl.ANY)] * count
    return pl.pallas_call(
        functools.partial(place_kernel, count),
        out_shape=[jax.ShapeDtypeStruct(a.shape, a.dtype) for a in arrays],
        in_specs=anywhere,
        out_specs=anywhere,
        scratch_shapes=[pltpu.VMEM(a.shape, a.dtype) for a in arrays] + [pltpu.SemaphoreType.DMA((count,))] * 2,
    )(*arrays)


def fused(n, models, *args):
    slopes, params, states = args[0:5], args[5:10], args[10:15]
    outer = n // INNER
    width = params[4].shape[0]
    row = lambda a: a.reshape(1, width)
    shapes = [p.shape for p in params[0:4]]
    f32 = lambda s: jax.ShapeDtypeStruct(s, jnp.float32)
    out_shape = (
        [jax.ShapeDtypeStruct(s.shape[1:], jnp.bfloat16) for s in slopes[0:4]]
        + [f32((n, 1, width))]
        + ([f32(s) for s in shapes] + [f32((1, width))]) * 2
    )
    dma = lambda *s: pltpu.SemaphoreType.DMA(s)
    scratch = (
        [pltpu.VMEM((outer,) + s, jnp.bfloat16) for s in shapes]
        + [pltpu.VMEM((outer,) + s, jnp.float32) for s in shapes] * 2
        + [pltpu.VMEM(s, jnp.float32) for s in shapes]
        + [pltpu.VMEM(s.shape[1:], jnp.bfloat16) for s in slopes[0:4]]
        + [pltpu.VMEM(s, jnp.float32) for s in shapes] * 2
        + [pltpu.VMEM(s.shape[1:], jnp.bfloat16) for s in slopes[0:4]]
        + [pltpu.VMEM(s, jnp.float32) for s in shapes] * 2
        + [
            pltpu.VMEM((models, 4, 8, shapes[0][0]), jnp.float32),
            pltpu.VMEM((4, models, 8, shapes[0][0]), jnp.float32),
            pltpu.VMEM(slopes[4].shape, jnp.float32),
            pltpu.VMEM((n, 1, width), jnp.float32),
        ]
        + [dma(4, outer)] * 12
        + [dma(models)] * 2
        + [dma(4, models)] * 2
        + [dma(n)] * 4
        + [dma(6, 4)]
    )
    specs = ([pl.BlockSpec(memory_space=pl.ANY)] * 4 + [pl.BlockSpec(memory_space=pltpu.VMEM)]) * 3
    outs = pl.pallas_call(
        functools.partial(kernel, n, models),
        out_shape=out_shape,
        in_specs=specs,
        out_specs=specs,
        scratch_shapes=scratch,
        compiler_params=pltpu.CompilerParams(collective_id=0, has_side_effects=True),
    )(*slopes, *params[0:4], row(params[4]), *states[0:4], row(states[4]))
    outs = list(outs)
    moved = [i for i in range(15) if i != 4]
    for i, a in zip(moved, placed([outs[i] for i in moved])):
        outs[i] = a
    outs[4] = outs[4].reshape(-1).astype(jnp.bfloat16)
    outs[9] = outs[9].reshape(-1)
    outs[14] = outs[14].reshape(-1)
    return tuple(outs)


def plain(*args):
    slopes, params, states = args[0:5], args[5:10], args[10:15]
    rate = lax.axis_size("replica") ** (-0.5)
    dims = (0, 0, 0, 1)
    means = [
        lax.psum_scatter(s[0].astype(jnp.float32), "replica", scatter_dimension=d, tiled=True) * rate
        for s, d in zip(slopes, dims)
    ]
    whole = lax.psum(slopes[4][0].astype(jnp.float32), "replica")
    width = params[4].shape[0]
    mean_norm = lax.dynamic_slice_in_dim(whole, lax.axis_index("replica") * width, width) * rate
    size = lambda a, d: jnp.sum(a * a, axis=1 - d, keepdims=True)
    own, got = lax.psum(
        ([size(p, d) for p, d in zip(params, dims)], [size(a, d) for a, d in zip(means, dims)]), "model"
    )
    means = [a * (jnp.sqrt(o) * lax.rsqrt(g + 1e-06)) for a, o, g in zip(means, own, got)] + [mean_norm]
    pairs = [updated(p, a, s) for p, a, s in zip(params, means, states)]
    halves = [
        lax.all_gather(v.astype(jnp.bfloat16), "replica", axis=d, tiled=True)
        for (v, _), d in zip(pairs, dims + (0,))
    ]
    return tuple(halves) + tuple(v for v, _ in pairs) + tuple(s for _, s in pairs)


def solution(mesh):
    n, models = mesh.shape["replica"], mesh.shape["model"]

    def local(*args):
        rows, columns, width = args[5].shape[0], args[8].shape[1], args[9].shape[0]
        aligned = rows % LANES == 0 and columns % LANES == 0 and width % LANES == 0
        if n % INNER == 0 and aligned and rows == columns:
            return fused(n, models, *args)
        return plain(*args)

    inner, turned = P("replica", "model"), P("model", "replica")
    slices = (P("replica", None, "model"),) * 3 + (P("replica", "model", None), P("replica", None))
    shares = (inner,) * 3 + (turned, P("replica"))
    return jax.shard_map(
        local,
        mesh=mesh,
        in_specs=slices + shares * 2,
        out_specs=(P(None, "model"),) * 3 + (P("model", None), P()) + shares * 2,
        check_vma=False,
    )
```
